32 devices in a mesh: tm: 8 (over z, core), member: 4 (over y, x).
Axes of the slice: x: 2, y: 2, z: 4, core: 2. Of those that a mesh axis runs over, the one named last changes fastest.
Arguments:
- fields: float32 [48, 48, 8192], P('member', 'tm'), may hold values from 200 to 350, as said below
Outputs:
- covariance: float32 [48, 48, 8192], P('member', None, 'tm')
The draws below stay inside these ranges and needn't reach their ends.
Inputs may be any that keep to these rules, and one draw needn't show every extreme that they name: `fields`: month t is calendar month t mod 12.
All inputs are finite; a program needn't handle non-finite values.
Results may differ from the reference program's by a relative error of at most 0.0003.
Values sent between devices are 32-bit elements; how exact they have to be, the bound alone decides.
No kernel may reach another device: no remote copies, remote signals or barrier semaphores. Data moves between devices by JAX's collectives and lax.ppermute only.
A program may use at most 192 MiB of HBM per device.

```python
import math
import jax
import jax.numpy as jnp
from jax import lax

MEMBERS = 48
MONTHS = 48
PIXELS = 8192


def draw_fields(key, part):
    subkeys = jax.random.split(key, 7)
    offset = jax.random.uniform(subkeys[0], (1, 1, PIXELS), jnp.float32, 250.0, 300.0)
    amplitude = jnp.exp(jax.random.uniform(subkeys[1], (1, 1, PIXELS), jnp.float32, 0.0, math.log(20.0)))
    phase_shift = jax.random.uniform(subkeys[2], (1, 1, PIXELS), jnp.float32, 0.0, 12.0)
    pixel_scale = jnp.exp(jax.random.uniform(subkeys[3], (1, 1, PIXELS), jnp.float32, math.log(0.3), math.log(3.0)))
    weight = jax.random.uniform(subkeys[4], (1, 1, PIXELS), jnp.float32, 0.6, 1.2)
    calendar = (jnp.arange(MONTHS) % 12).astype(jnp.float32).reshape(1, MONTHS, 1)
    season = amplitude * jnp.sin(2.0 * math.pi * (calendar + phase_shift) / 12.0)
    common = jax.random.normal(subkeys[5], (1, MONTHS, PIXELS), jnp.float32)
    member_noise = jax.random.normal(subkeys[6], (MEMBERS, MONTHS, PIXELS), jnp.float32)
    member_scale = jnp.ones((MEMBERS, 1, 1), jnp.float32)
    values = offset + season + pixel_scale * member_scale * (weight * common + member_noise)
    return jnp.clip(values, 200.0, 350.0).astype(jnp.float32)


def setup_inputs(seed: int = 0) -> dict:
    keys = jax.random.split(jax.random.key(seed), 2)
    return {
        "fields": draw_fields(jax.random.fold_in(keys[1], 71), 0),
    }


def monthly_anomaly(series):
    members_here, months_here, pixel_count = series.shape
    by_year = series.reshape(members_here, months_here // 12, 12, pixel_count)
    climatology = jnp.mean(by_year, axis=1, keepdims=True)
    return (by_year - climatology).reshape(members_here, months_here, pixel_count)


def reference(fields):
    anomaly = monthly_anomaly(fields)
    products = jnp.einsum("itp,jtp->ijp", anomaly, anomaly, precision=lax.Precision.HIGHEST, preferred_element_type=jnp.float32)
    return products / (MONTHS - 12)
```

```python
import functools
import math

import jax
import jax.numpy as jnp
from jax import lax
from jax.experimental import pallas as pl
from jax.experimental.pallas import tpu as pltpu
from jax.sharding import PartitionSpec as P

LANES = 128
YEAR = 12
VMEM_LIMIT = 48 * 1024 * 1024


def vmem_specs(count):
    return [pl.BlockSpec(memory_space=pltpu.VMEM)] * count


def pack_kernel(tm, block, widths, x_ref, *out_refs):
    me = lax.axis_index("tm")
    months = x_ref.shape[1]
    start = 0
    for c, width in enumerate(widths):
        for k in range(tm):
            first = pl.multiple_of((me ^ k) * block + start, LANES)
            for lane in range(0, width, LANES):
                lanes = pl.ds(pl.multiple_of(first + lane, LANES), LANES)
                out_refs[c * tm + k][:, lane : lane + LANES] = jnp.concatenate(
                    [x_ref[:, t, lanes] for t in range(months)], axis=0
                )
        start += width


def contrasts(by_year, norm):
    out = []
    for k in range(1, len(by_year)):
        total = by_year[k] - by_year[0]
        for j in range(1, k):
            total = total + (by_year[k] - by_year[j])
        out.append(total * (1.0 / math.sqrt(k * (k + 1) * norm)))
    return out


def contrast_kernel(halves, groups, norm, fold, *refs):
    tm = len(refs) - groups - (1 if fold > 1 else 0)
    in_refs, out_refs = refs[:tm], refs[tm : tm + groups]
    me = lax.axis_index("member")
    rows = in_refs[0].shape[0]
    years = tm // halves

    def at(lanes):
        return [
            contrasts([in_refs[y * halves + h][:, lanes] for y in range(years)], norm)
            for h in range(halves)
        ]

    if fold == 1:
        for d in range(groups):
            lanes = pl.ds(pl.multiple_of((me ^ d) * LANES, LANES), LANES)
            for h, values in enumerate(at(lanes)):
                for k, value in enumerate(values):
                    row = (k * halves + h) * rows
                    out_refs[d][row : row + rows, :] = value
        return
    held = refs[-1]
    part = LANES // fold
    low = lax.broadcasted_iota(jnp.int32, (rows, LANES), 1) < part
    for p in range(groups // fold):
        first, second = at(slice(p * LANES, (p + 1) * LANES))
        for k, (a, b) in enumerate(zip(first, second)):
            at_rows = slice(k * rows, (k + 1) * rows)
            held[2 * p, at_rows, :] = jnp.where(low, a, pltpu.roll(b, part, 1))
            held[2 * p + 1, at_rows, :] = jnp.where(low, pltpu.roll(a, part, 1), b)
    for d in range(groups):
        out_refs[d][...] = held[me ^ d]


def cov_kernel(groups, members, fold, *refs):
    in_refs, out_refs = refs[:groups], refs[groups : 2 * groups]
    held, joined, result = refs[2 * groups :]
    me = lax.axis_index("member")
    steps = in_refs[0].shape[0] // members
    whole = groups * members
    tiles = whole // 8
    for d in range(groups):
        held[me ^ d] = in_refs[d][...]
    for t in range(steps):
        joined[t] = jnp.concatenate(
            [held[m, t * members : (t + 1) * members, :] for m in range(groups)], axis=0
        )
    part = LANES // fold
    low = lax.broadcasted_iota(jnp.int32, (8, LANES), 1) < part
    planes = members // fold
    most = 4 // fold
    for m in range(groups):
        for a in range(0, planes, most):
            per = min(most, planes - a)
            rows = [m * members + a + s * planes + u for u in range(per) for s in range(fold)]

            def body(t, sums):
                right = [joined[t, 8 * j : 8 * j + 8, :] for j in range(tiles)]
                new = []
                for n, r in enumerate(rows):
                    left = jnp.broadcast_to(joined[t, r : r + 1, :], (8, LANES))
                    for j in range(tiles):
                        new.append(sums[n * tiles + j] + left * right[j])
                return tuple(new)

            zeros = tuple(jnp.zeros((8, LANES), jnp.float32) for _ in range(len(rows) * tiles))
            sums = lax.fori_loop(0, steps, body, zeros, unroll=3)
            for u in range(per):
                for j in range(tiles):
                    value = sums[u * fold * tiles + j]
                    if fold == 2:
                        other = sums[(u * fold + 1) * tiles + j]
                        value = jnp.where(
                            low, value + pltpu.roll(value, part, 1), other + pltpu.roll(other, part, 1)
                        )
                    result[m, a + u, 8 * j : 8 * j + 8, :] = value
    for d in range(groups):
        out_refs[d][...] = result[me ^ d]


def place_kernel(groups, fold, *refs):
    in_refs, out_ref = refs[:groups], refs[-1 - (1 if fold > 1 else 0)]
    me = lax.axis_index("member")
    if fold == 1:
        for d in range(groups):
            lanes = pl.ds(pl.multiple_of((me ^ d) * LANES, LANES), LANES)
            out_ref[:, :, lanes] = in_refs[d][...]
        return
    held = refs[-1]
    for d in range(groups):
        held[me ^ d] = in_refs[d][...]
    planes, whole = in_refs[0].shape[0], in_refs[0].shape[1]
    part = LANES // fold
    low = lax.broadcasted_iota(jnp.int32, (whole, LANES), 1) < part
    for p in range(groups // 2):
        lanes = slice(p * LANES, (p + 1) * LANES)
        for i in range(planes):
            a, b = held[2 * p, i], held[2 * p + 1, i]
            out_ref[i, :, lanes] = jnp.where(low, a, pltpu.roll(b, part, 1))
            out_ref[i + planes, :, lanes] = jnp.where(low, pltpu.roll(a, part, 1), b)


def chunk_widths(block, groups):
    whole, half = LANES * groups, LANES * groups // 2
    widths = [half, half] if block >= 2 * half else [block]
    while sum(widths) < block:
        widths.insert(0, min(whole, block - sum(widths)))
    return tuple(widths)


def params(**kw):
    return pltpu.CompilerParams(vmem_limit_bytes=VMEM_LIMIT, **kw)


def cost(flops, nbytes):
    return pl.CostEstimate(flops=int(flops), bytes_accessed=int(nbytes), transcendentals=0)


def swap(x, axis, size, k):
    return lax.ppermute(x, axis, [(i, i ^ k) for i in range(size)])


def per_device(fields):
    members, months, pixels = fields.shape
    tm, groups = lax.axis_size("tm"), lax.axis_size("member")
    halves = YEAR // months
    years = tm // halves
    block = pixels // tm
    widths = chunk_widths(block, groups)
    whole = members * groups
    rows = members * months
    norm = float(months * tm - YEAR)
    sd = lambda *s: jax.ShapeDtypeStruct(s, jnp.float32)

    packed = pl.pallas_call(
        functools.partial(pack_kernel, tm, block, widths),
        out_shape=[sd(rows, w) for w in widths for _ in range(tm)],
        in_specs=vmem_specs(1),
        out_specs=vmem_specs(tm * len(widths)),
        compiler_params=params(),
        cost_estimate=cost(4e6, 2 * fields.size * 4),
        name="pack",
    )(fields)

    order = sorted(range(1, tm), key=lambda k: (-(k // halves), k))
    arrived = []
    for c in range(len(widths)):
        mine = packed[c * tm : (c + 1) * tm]
        got = {k: swap(mine[k], "tm", tm, k) for k in order}
        arrived.append([mine[0]] + [got[k] for k in range(1, tm)])

    out = None
    start = 0
    for c, width in enumerate(widths):
        fold = LANES * groups // width
        total = (years - 1) * halves * rows // fold
        scratch = [pltpu.VMEM((groups, total, LANES), jnp.float32)]
        sent = pl.pallas_call(
            functools.partial(contrast_kernel, halves, groups, norm, fold),
            out_shape=[sd(total, LANES)] * groups,
            in_specs=vmem_specs(tm),
            out_specs=vmem_specs(groups),
            scratch_shapes=scratch if fold > 1 else [],
            compiler_params=params(),
            cost_estimate=cost(4e6, 8 * rows * tm * width),
            name="contrast",
        )(*arrived[c])
        here = [sent[0]] + [swap(sent[d], "member", groups, d) for d in range(1, groups)]
        planes = members // fold
        rows_out = pl.pallas_call(
            functools.partial(cov_kernel, groups, members, fold),
            out_shape=[sd(planes, whole, LANES)] * groups,
            in_specs=vmem_specs(groups),
            out_specs=vmem_specs(groups),
            scratch_shapes=scratch
            + [
                pltpu.VMEM((total // members, whole, LANES), jnp.float32),
                pltpu.VMEM((groups, planes, whole, LANES), jnp.float32),
            ],
            compiler_params=params(),
            cost_estimate=cost(1e7, 8 * total * groups * LANES),
            name="products",
        )(*here)
        parts = [rows_out[0]] + [swap(rows_out[d], "member", groups, d) for d in range(1, groups)]
        column = start // width
        out = pl.pallas_call(
            functools.partial(place_kernel, groups, fold),
            out_shape=sd(members, whole, block),
            grid=(1,),
            in_specs=vmem_specs(groups)
            + ([] if out is None else [pl.BlockSpec(memory_space=pl.ANY)]),
            out_specs=pl.BlockSpec((members, whole, width), lambda i, column=column: (0, 0, column)),
            scratch_shapes=(
                [pltpu.VMEM((groups, planes, whole, LANES), jnp.float32)] if fold > 1 else []
            ),
            input_output_aliases={} if out is None else {groups: 0},
            compiler_params=params(),
            cost_estimate=cost(1e6, 8 * members * whole * width),
            name="place",
        )(*parts, *([] if out is None else [out]))
        start += width
    return out


def solution(mesh):
    in_specs = (P("member", "tm", None),)
    out_specs = P("member", None, "tm")
    return jax.shard_map(
        per_device, mesh=mesh, in_specs=in_specs, out_specs=out_specs, check_vma=False
    )
```

```python
import functools
import math

import jax
import jax.numpy as jnp
from jax import lax
from jax.experimental import pallas as pl
from jax.experimental.pallas import tpu as pltpu
from jax.sharding import PartitionSpec as P


LANES = 128
YEAR = 12
VMEM_LIMIT = 48 * 1024 * 1024


def vmem_specs(count):
    return [pl.BlockSpec(memory_space=pltpu.VMEM)] * count


def pack_kernel(tm, groups, block, widths, x_ref, *refs):
    me = lax.axis_index("tm")
    at_group = lax.axis_index("member")
    members, months = x_ref.shape[0], x_ref.shape[1]

    def rows_of(lanes, steps):
        return jnp.concatenate([x_ref[:, t, lanes] for t in steps], axis=0)

    held = refs[-1]
    refs = list(refs[:-1])
    start = 0
    for c, width in enumerate(widths):
        if c == 0:
            outs, refs = refs[:tm], refs[tm:]
            for k in range(tm):
                for lane in range(0, width, LANES):
                    lanes = pl.ds(pl.multiple_of((me ^ k) * block + lane, LANES), LANES)
                    outs[k][:, lane : lane + LANES] = rows_of(lanes, range(months))
        else:
            outs, refs = refs[:groups], refs[groups:]
            fold = LANES * groups // width
            part, steps = LANES // fold, months // fold
            rows = members * steps
            low = lax.broadcasted_iota(jnp.int32, (rows, LANES), 1) < part
            for k in range(tm):
                at_rows = slice(k * rows, (k + 1) * rows)
                for p in range(groups // fold):
                    first = (me ^ k) * block + start + p * LANES
                    lanes = pl.ds(pl.multiple_of(first, LANES), LANES)
                    a = rows_of(lanes, range(steps))
                    if fold == 1:
                        held[p, at_rows, :] = a
                        continue
                    b = rows_of(lanes, range(steps, months))
                    held[2 * p, at_rows, :] = jnp.where(low, a, pltpu.roll(b, part, 1))
                    held[2 * p + 1, at_rows, :] = jnp.where(low, pltpu.roll(a, part, 1), b)
            for d in range(groups):
                outs[d][...] = held[at_group ^ d, : tm * rows, :]
        start += width


def repack_kernel(tm, groups, members, *refs):
    in_refs, out_refs, held = refs[:groups], refs[groups : groups + tm], refs[-1]
    me = lax.axis_index("member")
    whole = groups * members
    rows = in_refs[0].shape[0] // tm
    for d in range(groups):
        held[me ^ d] = in_refs[d][...]
    for k in range(tm):
        for t in range(rows // members):
            row = k * rows + t * members
            out_refs[k][t * whole : (t + 1) * whole, :] = jnp.concatenate(
                [held[m, row : row + members, :] for m in range(groups)], axis=0
            )


def contrasts(by_year, norm):
    out = []
    for k in range(1, len(by_year)):
        total = by_year[k] - by_year[0]
        for j in range(1, k):
            total = total + (by_year[k] - by_year[j])
        out.append(total * (1.0 / math.sqrt(k * (k + 1) * norm)))
    return out


def contrast_kernel(halves, groups, norm, fold, *refs):
    tm = len(refs) - groups - 2
    in_refs, out_refs = refs[:tm], refs[tm + 1 : tm + 1 + groups]
    me = lax.axis_index("member")
    rows = in_refs[0].shape[0]
    years = tm // halves

    def at(lanes):
        return [
            contrasts([in_refs[y * halves + h][:, lanes] for y in range(years)], norm)
            for h in range(halves)
        ]

    if fold == 1:
        for d in range(groups):
            lanes = pl.ds(pl.multiple_of((me ^ d) * LANES, LANES), LANES)
            for h, values in enumerate(at(lanes)):
                for k, value in enumerate(values):
                    row = (k * halves + h) * rows
                    out_refs[d][row : row + rows, :] = value
        return
    held = refs[-1]
    part = LANES // fold
    low = lax.broadcasted_iota(jnp.int32, (rows, LANES), 1) < part
    for p in range(groups // fold):
        first, second = at(slice(p * LANES, (p + 1) * LANES))
        for k, (a, b) in enumerate(zip(first, second)):
            at_rows = slice(k * rows, (k + 1) * rows)
            held[2 * p, at_rows, :] = jnp.where(low, a, pltpu.roll(b, part, 1))
            held[2 * p + 1, at_rows, :] = jnp.where(low, pltpu.roll(a, part, 1), b)
    for d in range(groups):
        out_refs[d][...] = held[me ^ d]


def products(groups, members, fold, joined, result):
    steps, whole = joined.shape[0], joined.shape[1]
    tiles = whole // 8
    part = LANES // fold
    low = lax.broadcasted_iota(jnp.int32, (8, LANES), 1) < part
    planes = members // fold
    most = 4 // fold
    for m in range(groups):
        for a in range(0, planes, most):
            per = min(most, planes - a)
            rows = [m * members + a + s * planes + u for u in range(per) for s in range(fold)]

            def body(t, sums):
                right = [joined[t, 8 * j : 8 * j + 8, :] for j in range(tiles)]
                new = []
                for n, r in enumerate(rows):
                    left = jnp.broadcast_to(joined[t, r : r + 1, :], (8, LANES))
                    for j in range(tiles):
                        new.append(sums[n * tiles + j] + left * right[j])
                return tuple(new)

            zeros = tuple(jnp.zeros((8, LANES), jnp.float32) for _ in range(len(rows) * tiles))
            sums = lax.fori_loop(0, steps, body, zeros, unroll=3)
            for u in range(per):
                for j in range(tiles):
                    value = sums[u * fold * tiles + j]
                    if fold == 2:
                        other = sums[(u * fold + 1) * tiles + j]
                        value = jnp.where(
                            low, value + pltpu.roll(value, part, 1), other + pltpu.roll(other, part, 1)
                        )
                    result[m, a + u, 8 * j : 8 * j + 8, :] = value


def group_products_kernel(groups, members, fold, *refs):
    in_refs, out_refs = refs[:groups], refs[groups : 2 * groups]
    held, joined, result = refs[2 * groups :]
    me = lax.axis_index("member")
    for d in range(groups):
        held[me ^ d] = in_refs[d][...]
    for t in range(joined.shape[0]):
        joined[t] = jnp.concatenate(
            [held[m, t * members : (t + 1) * members, :] for m in range(groups)], axis=0
        )
    products(groups, members, fold, joined, result)
    for d in range(groups):
        out_refs[d][...] = result[me ^ d]


def block_products_kernel(tm, halves, groups, members, norm, fold, *refs):
    in_refs, out_refs = refs[:tm], refs[tm : tm + groups]
    joined, result = refs[tm + groups :]
    me = lax.axis_index("member")
    whole = groups * members
    per_half = in_refs[0].shape[0] // whole
    for h in range(halves):
        for t in range(per_half):
            values = [in_refs[k][t * whole : (t + 1) * whole, :] for k in range(h, tm, halves)]
            for k, value in enumerate(contrasts(values, norm)):
                joined[(k * halves + h) * per_half + t] = value
    products(groups, members, fold, joined, result)
    for d in range(groups):
        out_refs[d][...] = result[me ^ d]


def place_kernel(groups, fold, *refs):
    in_refs, out_ref = refs[:groups], refs[-2]
    me = lax.axis_index("member")
    if fold == 1:
        for d in range(groups):
            lanes = pl.ds(pl.multiple_of((me ^ d) * LANES, LANES), LANES)
            out_ref[:, :, lanes] = in_refs[d][...]
        return
    held = refs[-1]
    for d in range(groups):
        held[me ^ d] = in_refs[d][...]
    planes, whole = in_refs[0].shape[0], in_refs[0].shape[1]
    part = LANES // fold
    low = lax.broadcasted_iota(jnp.int32, (whole, LANES), 1) < part
    for p in range(groups // 2):
        lanes = slice(p * LANES, (p + 1) * LANES)
        for i in range(planes):
            a, b = held[2 * p, i], held[2 * p + 1, i]
            out_ref[i, :, lanes] = jnp.where(low, a, pltpu.roll(b, part, 1))
            out_ref[i + planes, :, lanes] = jnp.where(low, pltpu.roll(a, part, 1), b)


def chunk_widths(block, groups):
    whole, half = LANES * groups, LANES * groups // 2
    widths = [half, half] if block >= 2 * half else [block]
    while sum(widths) < block:
        widths.insert(0, min(whole, block - sum(widths)))
    return tuple(widths)


def params(**kw):
    return pltpu.CompilerParams(vmem_limit_bytes=VMEM_LIMIT, **kw)


def cost(flops, nbytes):
    return pl.CostEstimate(flops=int(flops), bytes_accessed=int(nbytes), transcendentals=0)


def call(kernel, outs, flops, nbytes, *args, scratch=()):
    return pl.pallas_call(
        kernel,
        out_shape=[jax.ShapeDtypeStruct(o, jnp.float32) for o in outs],
        in_specs=vmem_specs(len(args)),
        out_specs=vmem_specs(len(outs)),
        scratch_shapes=[pltpu.VMEM(s, jnp.float32) for s in scratch],
        compiler_params=params(),
        cost_estimate=cost(flops, nbytes),
    )(*args)


def gate_kernel(x_ref, out_ref):
    out_ref[...] = x_ref[:8, :LANES]


def swap(x, axis, size, k):
    return lax.ppermute(x, axis, [(i, i ^ k) for i in range(size)])


def swap_all(pieces, axis, order):
    got = {k: swap(pieces[k], axis, len(pieces), k) for k in order}
    return [pieces[0]] + [got[k] for k in range(1, len(pieces))]


def per_device(fields):
    members, months, pixels = fields.shape
    tm, groups = lax.axis_size("tm"), lax.axis_size("member")
    halves = YEAR // months
    years = tm // halves
    block = pixels // tm
    widths = chunk_widths(block, groups)
    whole = members * groups
    rows = members * months
    norm = float(months * tm - YEAR)
    far_first = sorted(range(1, tm), key=lambda k: (-(k // halves), k))
    near = range(1, groups)
    folds = [LANES * groups // w for w in widths]
    count = len(widths)

    shapes = [(rows, widths[0])] * tm
    for c in range(1, count):
        shapes += [(tm * rows // folds[c], LANES)] * groups
    held = (groups, tm * rows // min(folds[1:], default=1), LANES)
    packed = call(
        functools.partial(pack_kernel, tm, groups, block, widths),
        shapes, 4e6, 2 * fields.size * 4, fields, scratch=[held],
    )
    by_block, packed = packed[:tm], packed[tm:]
    arrived = [swap_all(by_block, "tm", far_first)]
    near_in = [None] + [
        swap_all(packed[(c - 1) * groups : c * groups], "member", near)
        for c in range(1, count)
    ]
    for c in range(1, count):
        total = tm * rows // folds[c]
        mine = call(
            functools.partial(repack_kernel, tm, groups, members),
            [(total * groups // tm, LANES)] * tm, 1e6, 8 * total * groups * LANES,
            *near_in[c], scratch=[(groups, total, LANES)],
        )
        arrived.append(swap_all(mine, "tm", far_first))

    gate = call(gate_kernel, [(8, LANES)], 1e5, 8192, by_block[0])[0]

    out = None
    start = 0
    for c, width in enumerate(widths):
        fold = folds[c]
        planes = members // fold
        total = (years - 1) * halves * rows // fold
        result = [(planes, whole, LANES)] * groups
        tail = [(total // members, whole, LANES), (groups, planes, whole, LANES)]
        if c == 0:
            sent = call(
                functools.partial(contrast_kernel, halves, groups, norm, fold),
                [(total, LANES)] * groups, 4e6, 8 * rows * tm * width,
                *arrived[0], gate, scratch=[(groups, total, LANES)],
            )
            here = swap_all(sent, "member", near)
            summed = call(
                functools.partial(group_products_kernel, groups, members, fold),
                result, 1e7, 8 * total * groups * LANES,
                *here, scratch=[(groups, total, LANES)] + tail,
            )
        else:
            summed = call(
                functools.partial(block_products_kernel, tm, halves, groups, members, norm, fold),
                result, 1e7, 8 * total * groups * LANES,
                *arrived[c], scratch=tail,
            )
        parts = swap_all(summed, "member", near)
        column = start // width
        out = pl.pallas_call(
            functools.partial(place_kernel, groups, fold),
            out_shape=jax.ShapeDtypeStruct((members, whole, block), jnp.float32),
            grid=(1,),
            in_specs=vmem_specs(groups)
            + ([] if out is None else [pl.BlockSpec(memory_space=pl.ANY)]),
            out_specs=pl.BlockSpec((members, whole, width), lambda i, column=column: (0, 0, column)),
            scratch_shapes=[pltpu.VMEM((groups, planes, whole, LANES), jnp.float32)],
            input_output_aliases={} if out is None else {groups: 0},
            compiler_params=params(),
            cost_estimate=cost(1e6, 8 * members * whole * width),
        )(*parts, *([] if out is None else [out]))
        start += width
    return out


def solution(mesh):
    in_specs = (P("member", "tm", None),)
    out_specs = P("member", None, "tm")

    return jax.shard_map(per_device, mesh=mesh, in_specs=in_specs, out_specs=out_specs, check_vma=False)
```

```python
import functools
import math

import jax
import jax.numpy as jnp
from jax import lax
from jax.experimental import pallas as pl
from jax.experimental.pallas import tpu as pltpu
from jax.sharding import PartitionSpec as P


LANES = 128
FOLD = 2
PART = LANES // FOLD
YEAR = 12
VMEM_LIMIT = 48 * 1024 * 1024


def low_lanes(rows):
    return lax.broadcasted_iota(jnp.int32, (rows, LANES), 1) < PART


def split_lanes(a, b, low):
    return jnp.where(low, a, pltpu.roll(b, PART, 1)), jnp.where(low, pltpu.roll(a, PART, 1), b)


def pack_kernel(tm, halves, groups, block, width, chunks, x_ref, *refs):
    first_refs, kept_ref, other_ref, held = refs[:tm], refs[tm], refs[tm + 1], refs[tm + 2]
    me = lax.axis_index("tm")
    at_group = lax.axis_index("member")
    members, months = x_ref.shape[0], x_ref.shape[1]
    steps = months // FOLD
    rows = members * steps
    low = low_lanes(rows)

    def rows_of(k, lane, times):
        lanes = pl.ds(pl.multiple_of((me ^ k) * block + lane, LANES), LANES)
        return jnp.concatenate([x_ref[:, t, lanes] for t in times], axis=0)

    for k in range(tm):
        for lane in range(0, width, LANES):
            first_refs[k][:, lane : lane + LANES] = rows_of(k, lane, range(months))
    size = (tm // halves) * rows
    for c in range(1, chunks):
        for h, out_ref in enumerate((kept_ref, other_ref)):
            for y in range(tm // halves):
                at_rows = slice(y * rows, (y + 1) * rows)
                for p in range(groups // FOLD):
                    lane = c * width + p * LANES
                    a = rows_of(y * halves + h, lane, range(steps))
                    b = rows_of(y * halves + h, lane, range(steps, months))
                    held[FOLD * p, at_rows, :], held[FOLD * p + 1, at_rows, :] = split_lanes(a, b, low)
            for d in range(groups):
                row = ((c - 1) * groups + d) * size
                out_ref[row : row + size, :] = held[at_group ^ d]


def merge_kernel(groups, sets, kept_ref, other_ref, *out_refs):
    size = kept_ref.shape[0] // (groups * sum(len(s) for s in sets))
    for n, chunk_set in enumerate(sets):
        for d in range(groups):
            for i, c in enumerate(chunk_set):
                row = ((c - 1) * groups + d) * size
                for h, in_ref in enumerate((kept_ref, other_ref)):
                    to = (i * 2 + h) * size
                    out_refs[n * groups + d][to : to + size, :] = in_ref[row : row + size, :]


def repack_kernel(years, halves, groups, members, count, *refs):
    in_refs, out_refs, held = refs[:groups], refs[groups:-1], refs[-1]
    me = lax.axis_index("member")
    whole = groups * members
    rows = in_refs[0].shape[0] // (count * halves * years)
    steps = rows // members
    for d in range(groups):
        held[me ^ d] = in_refs[d][...]
    for c in range(count):
        for y in range(years):
            for h in range(halves):
                for t in range(steps):
                    row = ((c * halves + h) * years + y) * rows + t * members
                    to = (h * steps + t) * whole
                    out_refs[c * years + y][to : to + whole, :] = jnp.concatenate(
                        [held[m, row : row + members, :] for m in range(groups)], axis=0
                    )


def contrasts(by_year, norm):
    out = []
    for k in range(1, len(by_year)):
        total = by_year[k] - by_year[0]
        for j in range(1, k):
            total = total + (by_year[k] - by_year[j])
        out.append(total * (1.0 / math.sqrt(k * (k + 1) * norm)))
    return out


def contrast_kernel(halves, groups, norm, *refs):
    tm = len(refs) - groups - 2
    in_refs, out_refs, held = refs[:tm], refs[tm + 1 : tm + 1 + groups], refs[-1]
    me = lax.axis_index("member")
    rows = in_refs[0].shape[0]
    low = low_lanes(rows)
    for p in range(groups // FOLD):
        lanes = slice(p * LANES, (p + 1) * LANES)
        first, second = (
            contrasts([in_refs[k][:, lanes] for k in range(h, tm, halves)], norm) for h in range(halves)
        )
        for k, (a, b) in enumerate(zip(first, second)):
            at_rows = slice(k * rows, (k + 1) * rows)
            held[FOLD * p, at_rows, :], held[FOLD * p + 1, at_rows, :] = split_lanes(a, b, low)
    for d in range(groups):
        out_refs[d][...] = held[me ^ d]


def transposed(block):
    sublane = lax.broadcasted_iota(jnp.int32, (8, LANES), 0)
    for step in (4, 2, 1):
        keep = (sublane & step) == 0
        new = list(block)
        for s in range(8):
            if not s & step:
                a, b = block[s], block[s + step]
                new[s] = jnp.where(keep, a, pltpu.roll(b, step, 0))
                new[s + step] = jnp.where(keep, pltpu.roll(a, 8 - step, 0), b)
        block = new
    return block


def products(members, joined, full, out_refs):
    me = lax.axis_index("member")
    steps, whole = joined.shape[0], joined.shape[1]
    tiles = whole // 8
    low = low_lanes(8)
    planes = members // FOLD

    def at(row, tile):
        first = (row % members) * whole + 8 * tile
        return row // members, slice(first, first + 8), slice(None)

    for i in range(tiles):
        most = max(1, min(8, 24 // (tiles - i)))
        for first in range(0, 8, most):
            rows = range(8 * i + first, 8 * i + min(8, first + most))
            sums = {}
            for t in range(steps):
                right = {j: joined[t, 8 * j : 8 * j + 8, :] for j in range(i, tiles)}
                for r in rows:
                    left = jnp.broadcast_to(joined[t, r : r + 1, :], (8, LANES))
                    for j in range(i, tiles):
                        term = left * right[j]
                        sums[r, j] = term if t == 0 else sums[r, j] + term
            for (r, j), x in sums.items():
                full[at(r, j)] = x + pltpu.roll(x, PART, 1)
    for i in range(tiles):
        for j in range(i + 1, tiles):
            block = [full[at(8 * i + s, j)] for s in range(8)]
            for s, value in enumerate(transposed(block)):
                full[at(8 * j + s, i)] = value
    for d in range(len(out_refs)):
        m = me ^ d
        for a in range(planes):
            for j in range(tiles):
                x, y = (full[m, u * whole + 8 * j : u * whole + 8 * j + 8, :] for u in (a, a + planes))
                out_refs[d][a, 8 * j : 8 * j + 8, :] = jnp.where(low, x, y)


def group_products_kernel(groups, members, *refs):
    in_refs, out_refs = refs[:groups], refs[groups : 2 * groups]
    held, joined, full = refs[2 * groups :]
    me = lax.axis_index("member")
    for d in range(groups):
        held[me ^ d] = in_refs[d][...]
    for t in range(joined.shape[0]):
        joined[t] = jnp.concatenate(
            [held[m, t * members : (t + 1) * members, :] for m in range(groups)], axis=0
        )
    products(members, joined, full, out_refs)


def fill(joined, in_refs, whole, norm):
    per_year = in_refs[0].shape[0] // whole
    for t in range(per_year):
        values = [in_ref[t * whole : (t + 1) * whole, :] for in_ref in in_refs]
        for k, value in enumerate(contrasts(values, norm)):
            joined[k * per_year + t] = value


def block_products_kernel(years, groups, members, norm, *refs):
    in_refs, out_refs = refs[:years], refs[years : years + groups]
    joined, full = refs[years + groups :]
    fill(joined, in_refs, groups * members, norm)
    products(members, joined, full, out_refs)


def farthest_products_kernel(years, groups, members, norm, *refs):
    in_refs, joined, out_ref = refs[:years], refs[years], refs[years + 1]
    fill(joined, in_refs, groups * members, norm)
    first = (lax.axis_index("member") ^ (groups - 1)) * members
    planes, tiles = members // FOLD, groups * members // 8
    low = low_lanes(8)
    for a in range(0, planes, 2):
        rows = [u + s * planes for u in range(a, min(a + 2, planes)) for s in range(FOLD)]
        sums = {}
        for t in range(joined.shape[0]):
            right = [joined[t, 8 * j : 8 * j + 8, :] for j in range(tiles)]
            for r in rows:
                left = jnp.broadcast_to(joined[t, pl.ds(first + r, 1), :], (8, LANES))
                for j in range(tiles):
                    term = left * right[j]
                    sums[r, j] = term if t == 0 else sums[r, j] + term
        for u in range(a, min(a + 2, planes)):
            for j in range(tiles):
                x, y = sums[u, j], sums[u + planes, j]
                out_ref[u, 8 * j : 8 * j + 8, :] = jnp.where(
                    low, x + pltpu.roll(x, PART, 1), y + pltpu.roll(y, PART, 1)
                )


def other_products_kernel(members, *refs):
    products(members, refs[0], refs[-1], refs[1:-1])


def place_kernel(groups, *refs):
    in_refs, out_ref, held = refs[:groups], refs[-2], refs[-1]
    me = lax.axis_index("member")
    for d in range(groups):
        held[me ^ d] = in_refs[d][...]
    planes, whole = in_refs[0].shape[0], in_refs[0].shape[1]
    low = low_lanes(whole)
    for p in range(groups // FOLD):
        lanes = slice(p * LANES, (p + 1) * LANES)
        for i in range(planes):
            out_ref[i, :, lanes], out_ref[i + planes, :, lanes] = split_lanes(
                held[FOLD * p, i], held[FOLD * p + 1, i], low
            )


def call(kernel, outs, flops, *args, scratch=()):
    nbytes = 4 * (sum(math.prod(o) for o in outs) + sum(a.size for a in args))
    return pl.pallas_call(
        kernel,
        out_shape=[jax.ShapeDtypeStruct(o, jnp.float32) for o in outs],
        in_specs=[pl.BlockSpec(memory_space=pltpu.VMEM)] * len(args),
        out_specs=[pl.BlockSpec(memory_space=pltpu.VMEM)] * len(outs),
        scratch_shapes=[pltpu.VMEM(s, jnp.float32) for s in scratch],
        compiler_params=pltpu.CompilerParams(vmem_limit_bytes=VMEM_LIMIT),
        cost_estimate=pl.CostEstimate(flops=int(flops), bytes_accessed=nbytes, transcendentals=0),
    )(*args)


def gate_kernel(x_ref, out_ref):
    out_ref[...] = x_ref[:8, :LANES]


def swap(x, axis, k):
    return lax.ppermute(x, axis, [(i, i ^ k) for i in range(lax.axis_size(axis))])


def swap_all(pieces, axis, stride):
    out = dict(enumerate(pieces[:1]))
    for k in reversed(range(1, len(pieces))):
        out[k] = swap(pieces[k], axis, k * stride)
    return [out[k] for k in range(len(pieces))]


def chunk_sets(chunks):
    sets = [[1], list(range(2, chunks))]
    return [s for s in sets if s]


def per_device(fields):
    members, months, pixels = fields.shape
    tm, groups = lax.axis_size("tm"), lax.axis_size("member")
    halves = YEAR // months
    years = tm // halves
    block = pixels // tm
    width = PART * groups
    chunks = block // width
    whole = members * groups
    rows = members * months
    part_rows = rows // FOLD
    norm = float(months * tm - YEAR)
    sets = chunk_sets(chunks)
    assert halves == 2 and months % FOLD == 0 and members % FOLD == 0 and block == chunks * width

    both = ((chunks - 1) * groups * years * part_rows, LANES)
    packed = call(
        functools.partial(pack_kernel, tm, halves, groups, block, width, chunks),
        [(rows, width)] * tm + [both] * 2, 4e6, fields,
        scratch=[(groups, years * part_rows, LANES)],
    )
    by_block, kept, other = packed[:tm], packed[tm], packed[tm + 1]
    other = swap(other, "tm", 1)
    arrived = {0: by_block[0]}
    for k in sorted(range(1, tm), key=lambda k: (-(k // halves), k)):
        far = k >= tm - halves
        arrived[k] = swap(by_block[k], "tm", k)
    arrived = [arrived[k] for k in range(tm)]

    merged = call(
        functools.partial(merge_kernel, groups, sets),
        [(len(s) * halves * years * part_rows, LANES) for s in sets for _ in range(groups)],
        1e6, kept, other,
    )
    by_year = {}
    for n, chunk_set in enumerate(sets):
        near = swap_all(merged[n * groups : (n + 1) * groups], "member", 1)
        mine = call(
            functools.partial(repack_kernel, years, halves, groups, members, len(chunk_set)),
            [(halves * part_rows * groups, LANES)] * (years * len(chunk_set)),
            1e6, *near, scratch=[(groups, *near[0].shape)],
        )
        for i, c in enumerate(chunk_set):
            by_year[c] = swap_all(mine[i * years : (i + 1) * years], "tm", halves)

    gate = call(gate_kernel, [(8, LANES)], 1e5, by_block[0])[0]
    total = (years - 1) * halves * part_rows
    result = [(members // FOLD, whole, LANES)] * groups
    tail = [(total // members, whole, LANES), (groups, members * whole, LANES)]
    parts = []
    for c in range(chunks):
        if c == 0:
            sent = call(
                functools.partial(contrast_kernel, halves, groups, norm),
                [(total, LANES)] * groups, 4e6, *arrived, gate,
                scratch=[(groups, total, LANES)],
            )
            here = swap_all(sent, "member", 1)
            summed = call(
                functools.partial(group_products_kernel, groups, members),
                result, 1e7, *here, scratch=[(groups, total, LANES)] + tail,
            )
        elif c == chunks - 1:
            joined, far = call(
                functools.partial(farthest_products_kernel, years, groups, members, norm),
                [tail[0], result[0]], 3e6, *by_year[c],
            )
            far = swap(far, "member", groups - 1)
            summed = call(
                functools.partial(other_products_kernel, members),
                result[1:], 1e7, joined, scratch=tail[1:],
            )
            parts.append(swap_all(summed, "member", 1) + [far])
            continue
        else:
            summed = call(
                functools.partial(block_products_kernel, years, groups, members, norm),
                result, 1e7, *by_year[c], scratch=tail,
            )
        parts.append(swap_all(summed, "member", 1))

    out = []
    for c in range(chunks):
        out = [
            pl.pallas_call(
                functools.partial(place_kernel, groups),
                out_shape=jax.ShapeDtypeStruct((members, whole, block), jnp.float32),
                grid=(1,),
                in_specs=[pl.BlockSpec(memory_space=pltpu.VMEM)] * groups
                + [pl.BlockSpec(memory_space=pl.ANY)] * len(out),
                out_specs=pl.BlockSpec((members, whole, width), lambda i, c=c: (0, 0, c)),
                scratch_shapes=[pltpu.VMEM((groups, members // FOLD, whole, LANES), jnp.float32)],
                input_output_aliases={groups: 0} if out else {},
                compiler_params=pltpu.CompilerParams(vmem_limit_bytes=VMEM_LIMIT),
                cost_estimate=pl.CostEstimate(
                    flops=1000000, bytes_accessed=8 * members * whole * width, transcendentals=0
                ),
            )(*parts[c], *out)
        ]
    return out[0]


def solution(mesh):
    in_specs = (P("member", "tm", None),)
    out_specs = P("member", None, "tm")

    return jax.shard_map(per_device, mesh=mesh, in_specs=in_specs, out_specs=out_specs, check_vma=False)
```

```python
import functools
import math

import jax
import jax.numpy as jnp
from jax import lax
from jax.experimental import pallas as pl
from jax.experimental.pallas import tpu as pltpu
from jax.sharding import PartitionSpec as P


LANES = 128
FOLD = 2
PART = LANES // FOLD
YEAR = 12
VMEM_LIMIT = 48 * 1024 * 1024
PACK_LIMIT = 50 * 1024 * 1024


def low_lanes(rows):
    return lax.broadcasted_iota(jnp.int32, (rows, LANES), 1) < PART


def split_lanes(a, b, low):
    return jnp.where(low, a, pltpu.roll(b, PART, 1)), jnp.where(low, pltpu.roll(a, PART, 1), b)


def pack_kernel(tm, halves, groups, block, width, chunks, x_ref, *refs):
    first_refs, kept_ref, other_ref = refs[:tm], refs[tm], refs[tm + 1]
    held, own, sems = refs[tm + 2 :]
    me = lax.axis_index("tm")
    at_group = lax.axis_index("member")
    members, months = x_ref.shape[0], x_ref.shape[1]
    steps = months // FOLD
    rows = members * steps
    low = low_lanes(rows)

    def rows_of(k, lane, times):
        lanes = slice(lane, lane + LANES)
        return jnp.concatenate([own[k, :, t, lanes] for t in times], axis=0)

    def copy(k):
        lanes = pl.ds(pl.multiple_of((me ^ k) * block, LANES), block)
        return pltpu.make_async_copy(x_ref.at[:, :, lanes], own.at[k], sems.at[k])

    for k in range(tm):
        copy(k).start()
    size = (tm // halves) * rows
    for k in range(tm):
        copy(k).wait()
        for lane in range(0, width, LANES):
            first_refs[k][:, lane : lane + LANES] = rows_of(k, lane, range(months))
        y, h = divmod(k, halves)
        at_rows = slice(y * rows, (y + 1) * rows)
        for c in range(1, chunks):
            at = h * (chunks - 1) + c - 1
            for p in range(groups // FOLD):
                lane = c * width + p * LANES
                a = rows_of(k, lane, range(steps))
                b = rows_of(k, lane, range(steps, months))
                a, b = split_lanes(a, b, low)
                held[at, FOLD * p, at_rows, :], held[at, FOLD * p + 1, at_rows, :] = a, b
    for h, out_ref in enumerate((kept_ref, other_ref)):
        for c in range(1, chunks):
            for d in range(groups):
                row = ((c - 1) * groups + d) * size
                out_ref[row : row + size, :] = held[h * (chunks - 1) + c - 1, at_group ^ d]


def merge_kernel(groups, sets, kept_ref, other_ref, *out_refs):
    size = kept_ref.shape[0] // (groups * sum(len(s) for s in sets))
    for n, chunk_set in enumerate(sets):
        for d in range(groups):
            for i, c in enumerate(chunk_set):
                row = ((c - 1) * groups + d) * size
                for h, in_ref in enumerate((kept_ref, other_ref)):
                    to = (i * 2 + h) * size
                    out_refs[n * groups + d][to : to + size, :] = in_ref[row : row + size, :]


def repack_kernel(years, halves, groups, members, count, *refs):
    in_refs, out_refs, held = refs[:groups], refs[groups:-1], refs[-1]
    me = lax.axis_index("member")
    whole = groups * members
    rows = in_refs[0].shape[0] // (count * halves * years)
    steps = rows // members
    for d in range(groups):
        held[me ^ d] = in_refs[d][...]
    for c in range(count):
        for y in range(years):
            for h in range(halves):
                for t in range(steps):
                    row = ((c * halves + h) * years + y) * rows + t * members
                    to = (h * steps + t) * whole
                    out_refs[c * years + y][to : to + whole, :] = jnp.concatenate(
                        [held[m, row : row + members, :] for m in range(groups)], axis=0
                    )


def contrasts(by_year, norm):
    out = []
    for k in range(1, len(by_year)):
        total = by_year[k] - by_year[0]
        for j in range(1, k):
            total = total + (by_year[k] - by_year[j])
        out.append(total * (1.0 / math.sqrt(k * (k + 1) * norm)))
    return out


def contrast_kernel(halves, groups, norm, *refs):
    tm = len(refs) - groups - 2
    in_refs, out_refs, held = refs[:tm], refs[tm + 1 : tm + 1 + groups], refs[-1]
    me = lax.axis_index("member")
    rows = in_refs[0].shape[0]
    low = low_lanes(rows)
    for p in range(groups // FOLD):
        lanes = slice(p * LANES, (p + 1) * LANES)
        first, second = (
            contrasts([in_refs[k][:, lanes] for k in range(h, tm, halves)], norm) for h in range(halves)
        )
        for k, (a, b) in enumerate(zip(first, second)):
            at_rows = slice(k * rows, (k + 1) * rows)
            held[FOLD * p, at_rows, :], held[FOLD * p + 1, at_rows, :] = split_lanes(a, b, low)
    for d in range(groups):
        out_refs[d][...] = held[me ^ d]


def transposed(block):
    sublane = lax.broadcasted_iota(jnp.int32, (8, LANES), 0)
    for step in (4, 2, 1):
        keep = (sublane & step) == 0
        new = list(block)
        for s in range(8):
            if not s & step:
                a, b = block[s], block[s + step]
                new[s] = jnp.where(keep, a, pltpu.roll(b, step, 0))
                new[s + step] = jnp.where(keep, pltpu.roll(a, 8 - step, 0), b)
        block = new
    return block


def products(members, joined, full, out_refs):
    me = lax.axis_index("member")
    steps, whole = joined.shape[0], joined.shape[1]
    tiles = whole // 8
    low = low_lanes(8)
    planes = members // FOLD

    def at(row, tile):
        first = (row % members) * whole + 8 * tile
        return row // members, slice(first, first + 8), slice(None)

    for i in range(tiles):
        most = max(1, min(8, 24 // (tiles - i)))
        for first in range(0, 8, most):
            rows = range(8 * i + first, 8 * i + min(8, first + most))
            sums = {}
            for t in range(steps):
                right = {j: joined[t, 8 * j : 8 * j + 8, :] for j in range(i, tiles)}
                for r in rows:
                    left = jnp.broadcast_to(joined[t, r : r + 1, :], (8, LANES))
                    for j in range(i, tiles):
                        term = left * right[j]
                        sums[r, j] = term if t == 0 else sums[r, j] + term
            for (r, j), x in sums.items():
                full[at(r, j)] = x + pltpu.roll(x, PART, 1)
    for i in range(tiles):
        for j in range(i + 1, tiles):
            block = [full[at(8 * i + s, j)] for s in range(8)]
            for s, value in enumerate(transposed(block)):
                full[at(8 * j + s, i)] = value
    for d in range(len(out_refs)):
        m = me ^ d
        for a in range(planes):
            for j in range(tiles):
                x, y = (full[m, u * whole + 8 * j : u * whole + 8 * j + 8, :] for u in (a, a + planes))
                out_refs[d][a, 8 * j : 8 * j + 8, :] = jnp.where(low, x, y)


def group_products_kernel(groups, members, *refs):
    in_refs, out_refs = refs[:groups], refs[groups : 2 * groups]
    held, joined, full = refs[2 * groups :]
    me = lax.axis_index("member")
    for d in range(groups):
        held[me ^ d] = in_refs[d][...]
    for t in range(joined.shape[0]):
        joined[t] = jnp.concatenate(
            [held[m, t * members : (t + 1) * members, :] for m in range(groups)], axis=0
        )
    products(members, joined, full, out_refs)


def fill(joined, in_refs, whole, norm):
    per_year = in_refs[0].shape[0] // whole
    for t in range(per_year):
        values = [in_ref[t * whole : (t + 1) * whole, :] for in_ref in in_refs]
        for k, value in enumerate(contrasts(values, norm)):
            joined[k * per_year + t] = value


def block_products_kernel(years, groups, members, norm, *refs):
    in_refs, out_refs = refs[:years], refs[years : years + groups]
    joined, full = refs[years + groups :]
    fill(joined, in_refs, groups * members, norm)
    products(members, joined, full, out_refs)


def farthest_products_kernel(years, groups, members, norm, *refs):
    in_refs, joined, out_ref = refs[:years], refs[years], refs[years + 1]
    fill(joined, in_refs, groups * members, norm)
    first = (lax.axis_index("member") ^ (groups - 1)) * members
    planes, tiles = members // FOLD, groups * members // 8
    low = low_lanes(8)
    for a in range(0, planes, 2):
        rows = [u + s * planes for u in range(a, min(a + 2, planes)) for s in range(FOLD)]
        sums = {}
        for t in range(joined.shape[0]):
            right = [joined[t, 8 * j : 8 * j + 8, :] for j in range(tiles)]
            for r in rows:
                left = jnp.broadcast_to(joined[t, pl.ds(first + r, 1), :], (8, LANES))
                for j in range(tiles):
                    term = left * right[j]
                    sums[r, j] = term if t == 0 else sums[r, j] + term
        for u in range(a, min(a + 2, planes)):
            for j in range(tiles):
                x, y = sums[u, j], sums[u + planes, j]
                out_ref[u, 8 * j : 8 * j + 8, :] = jnp.where(
                    low, x + pltpu.roll(x, PART, 1), y + pltpu.roll(y, PART, 1)
                )


def other_products_kernel(members, *refs):
    products(members, refs[0], refs[-1], refs[1:-1])


def place_kernel(groups, *refs):
    in_refs, out_ref, held = refs[:groups], refs[-2], refs[-1]
    me = lax.axis_index("member")
    for d in range(groups):
        held[me ^ d] = in_refs[d][...]
    planes, whole = in_refs[0].shape[0], in_refs[0].shape[1]
    low = low_lanes(whole)
    for p in range(groups // FOLD):
        lanes = slice(p * LANES, (p + 1) * LANES)
        for i in range(planes):
            out_ref[i, :, lanes], out_ref[i + planes, :, lanes] = split_lanes(
                held[FOLD * p, i], held[FOLD * p + 1, i], low
            )


def call(kernel, outs, flops, *args, scratch=()):
    nbytes = 4 * (sum(math.prod(o) for o in outs) + sum(a.size for a in args))
    return pl.pallas_call(
        kernel,
        out_shape=[jax.ShapeDtypeStruct(o, jnp.float32) for o in outs],
        in_specs=[pl.BlockSpec(memory_space=pltpu.VMEM)] * len(args),
        out_specs=[pl.BlockSpec(memory_space=pltpu.VMEM)] * len(outs),
        scratch_shapes=[pltpu.VMEM(s, jnp.float32) for s in scratch],
        compiler_params=pltpu.CompilerParams(vmem_limit_bytes=VMEM_LIMIT),
        cost_estimate=pl.CostEstimate(flops=int(flops), bytes_accessed=nbytes, transcendentals=0),
    )(*args)


def gate_kernel(x_ref, out_ref):
    out_ref[...] = x_ref[:8, :LANES]


def swap(x, axis, k):
    return lax.ppermute(x, axis, [(i, i ^ k) for i in range(lax.axis_size(axis))])


def swap_all(pieces, axis, stride):
    out = dict(enumerate(pieces[:1]))
    for k in reversed(range(1, len(pieces))):
        out[k] = swap(pieces[k], axis, k * stride)
    return [out[k] for k in range(len(pieces))]


def chunk_sets(chunks):
    sets = [[1], list(range(2, chunks))]
    return [s for s in sets if s]


def per_device(fields):
    members, months, pixels = fields.shape
    tm, groups = lax.axis_size("tm"), lax.axis_size("member")
    halves = YEAR // months
    years = tm // halves
    block = pixels // tm
    width = PART * groups
    chunks = block // width
    whole = members * groups
    rows = members * months
    part_rows = rows // FOLD
    norm = float(months * tm - YEAR)
    sets = chunk_sets(chunks)
    assert halves == 2 and months % FOLD == 0 and members % FOLD == 0 and block == chunks * width

    both = ((chunks - 1) * groups * years * part_rows, LANES)
    packed = pl.pallas_call(
        functools.partial(pack_kernel, tm, halves, groups, block, width, chunks),
        out_shape=[jax.ShapeDtypeStruct((rows, width), jnp.float32)] * tm
        + [jax.ShapeDtypeStruct(both, jnp.float32)] * 2,
        in_specs=[pl.BlockSpec(memory_space=pl.ANY)],
        out_specs=[pl.BlockSpec(memory_space=pltpu.VMEM)] * (tm + 2),
        scratch_shapes=[
            pltpu.VMEM((halves * (chunks - 1), groups, years * part_rows, LANES), jnp.float32),
            pltpu.VMEM((tm, members, months, block), jnp.float32),
            pltpu.SemaphoreType.DMA((tm,)),
        ],
        compiler_params=pltpu.CompilerParams(vmem_limit_bytes=PACK_LIMIT),
        cost_estimate=pl.CostEstimate(flops=4000000, bytes_accessed=8 * fields.size, transcendentals=0),
        name="pack",
    )(fields)
    by_block, kept, other = packed[:tm], packed[tm], packed[tm + 1]
    other = swap(other, "tm", 1)
    arrived = {0: by_block[0]}
    for k in sorted(range(1, tm), key=lambda k: (-(k // halves), k)):
        far = k >= tm - halves or k == tm - halves - 1
        arrived[k] = swap(by_block[k], "tm", k)
    arrived = [arrived[k] for k in range(tm)]

    merged = call(
        functools.partial(merge_kernel, groups, sets),
        [(len(s) * halves * years * part_rows, LANES) for s in sets for _ in range(groups)],
        1e6, kept, other,
    )
    by_year = {}
    for n, chunk_set in enumerate(sets):
        near = swap_all(merged[n * groups : (n + 1) * groups], "member", 1)
        mine = call(
            functools.partial(repack_kernel, years, halves, groups, members, len(chunk_set)),
            [(halves * part_rows * groups, LANES)] * (years * len(chunk_set)),
            1e6, *near, scratch=[(groups, *near[0].shape)],
        )
        for i, c in enumerate(chunk_set):
            by_year[c] = swap_all(mine[i * years : (i + 1) * years], "tm", halves)

    gate = call(gate_kernel, [(8, LANES)], 1e5, by_block[0])[0]
    total = (years - 1) * halves * part_rows
    result = [(members // FOLD, whole, LANES)] * groups
    tail = [(total // members, whole, LANES), (groups, members * whole, LANES)]
    parts = []
    for c in range(chunks):
        if c == 0:
            sent = call(
                functools.partial(contrast_kernel, halves, groups, norm),
                [(total, LANES)] * groups, 4e6, *arrived, gate,
                scratch=[(groups, total, LANES)],
            )
            here = swap_all(sent, "member", 1)
            summed = call(
                functools.partial(group_products_kernel, groups, members),
                result, 1e7, *here, scratch=[(groups, total, LANES)] + tail,
            )
        elif c == chunks - 1:
            joined, far = call(
                functools.partial(farthest_products_kernel, years, groups, members, norm),
                [tail[0], result[0]], 3e6, *by_year[c],
            )
            far = swap(far, "member", groups - 1)
            summed = call(
                functools.partial(other_products_kernel, members),
                result[1:], 1e7, joined, scratch=tail[1:],
            )
            parts.append(swap_all(summed, "member", 1) + [far])
            continue
        else:
            summed = call(
                functools.partial(block_products_kernel, years, groups, members, norm),
                result, 1e7, *by_year[c], scratch=tail,
            )
        parts.append(swap_all(summed, "member", 1))

    out = []
    for c in range(chunks):
        out = [
            pl.pallas_call(
                functools.partial(place_kernel, groups),
                out_shape=jax.ShapeDtypeStruct((members, whole, block), jnp.float32),
                grid=(1,),
                in_specs=[pl.BlockSpec(memory_space=pltpu.VMEM)] * groups
                + [pl.BlockSpec(memory_space=pl.ANY)] * len(out),
                out_specs=pl.BlockSpec((members, whole, width), lambda i, c=c: (0, 0, c)),
                scratch_shapes=[pltpu.VMEM((groups, members // FOLD, whole, LANES), jnp.float32)],
                input_output_aliases={groups: 0} if out else {},
                compiler_params=pltpu.CompilerParams(vmem_limit_bytes=VMEM_LIMIT),
                cost_estimate=pl.CostEstimate(
                    flops=1000000, bytes_accessed=8 * members * whole * width, transcendentals=0
                ),
            )(*parts[c], *out)
        ]
    return out[0]


def solution(mesh):
    in_specs = (P("member", "tm", None),)
    out_specs = P("member", None, "tm")

    return jax.shard_map(per_device, mesh=mesh, in_specs=in_specs, out_specs=out_specs, check_vma=False)
```
